32 devices in a mesh: group: 2 (over y), tensor: 4 (over z), seq: 4 (over x, core).
Axes of the slice: x: 2, y: 2, z: 4, core: 2. Of those that a mesh axis runs over, the one named last changes fastest.
Arguments:
- mixer_input: bfloat16 [2048, 8192], P(('group', 'seq'), 'tensor'), parts along dimension 0, may hold values from -6 to 6
- state_maps: bfloat16 [2048, 256], P(('group', 'seq')), parts along dimension 0, may hold values from -6 to 6
- gate_input: bfloat16 [2048, 8192], P(('group', 'seq'), 'tensor'), parts along dimension 0, may hold values from -6 to 6
- step_raw: float32 [128, 2048], P('tensor', ('group', 'seq')), parts along dimension 1, may hold values from -10 to 10, as said below
- decay_log: float32 [128], P('tensor'), may hold values from -4 to -2
- skip_gain: float32 [128], P('tensor'), may hold values from 0.5 to 1.5
- conv_input: bfloat16 [4, 8192], P(None, 'tensor'), may hold values from -3 to 3
- conv_maps: bfloat16 [4, 256], replicated, may hold values from -3 to 3
- norm_gain: float32 [8192], P('tensor'), may hold values from 0.1 to 1.9
- out_weight: bfloat16 [8192, 8192], P('tensor'), may hold values from -0.09375 to 0.09375
Outputs:
- mixed: bfloat16 [2048, 8192], P(('group', 'seq'), 'tensor'), parts along dimension 0
The draws below stay inside these ranges and needn't reach their ends.
There are 2 independent parts, one for each index of `group`. The reference program is written for one: setup_inputs(seed, part) draws one part's arguments, and reference() takes and returns one part's arrays. A program takes and returns all parts, laid end to end along the dimension named above; an argument that names none is the same for every part. Nothing has to cross between parts.
Inputs may be any that keep to these rules, and one draw needn't show every extreme that they name: `step_raw`: Real-valued step parameters before softplus.
All inputs are finite; a program needn't handle non-finite values.
Results may differ from the reference program's by a relative error of at most 0.008.
Values may be sent and summed in bfloat16 or wider, within the bound.
A program may use at most 128 MiB of HBM per device.

```python
import jax
import jax.numpy as jnp
from jax import lax

D = 8192
HEAD_TOTAL = 128
HEAD_DIM = 64
STATE = 128
CONV = 4
SPAN = 256
TOKENS_PER_SHARD = 256
INNER = 8192
SEQUENCE_LENGTH = 1024


def draw_step_raw(key, part):
    tensor_dims = (HEAD_TOTAL, SEQUENCE_LENGTH)
    kind_key = jax.random.fold_in(key, 31)
    slow_key = jax.random.fold_in(key, 32)
    fast_key = jax.random.fold_in(key, 33)
    spike_frequency_key = jax.random.fold_in(key, 34)
    spike_location_key = jax.random.fold_in(key, 35)
    spike_magnitude_key = jax.random.fold_in(key, 36)
    share_fast = 0.5
    fast_heads = jax.random.uniform(kind_key, (HEAD_TOTAL, 1), jnp.float32) < share_fast
    gradual_baseline = jax.random.uniform(slow_key, tensor_dims, jnp.float32, -9.0, -7.0)
    fast_base = jax.random.uniform(fast_key, tensor_dims, jnp.float32, 0.0, 3.0)
    segment_pieces = SEQUENCE_LENGTH // TOKENS_PER_SHARD
    segment_frequency = jax.random.uniform(spike_frequency_key, (HEAD_TOTAL, segment_pieces, 1), jnp.float32, 0.0, 3.0) / TOKENS_PER_SHARD
    position_frequency = jnp.broadcast_to(segment_frequency, (HEAD_TOTAL, segment_pieces, TOKENS_PER_SHARD)).reshape(tensor_dims)
    spike_events = jax.random.uniform(spike_location_key, tensor_dims, jnp.float32) < position_frequency
    spike_amounts = jax.random.uniform(spike_magnitude_key, tensor_dims, jnp.float32, 4.0, 6.0)
    gradual_amounts = jnp.where(spike_events, spike_amounts, gradual_baseline)
    return jnp.where(fast_heads, fast_base, gradual_amounts).astype(jnp.float32)


def spiked(array, key, source, target, parts, factor):
    owner, partner = [(jnp.arange(array.shape[dim]) // (array.shape[dim] // parts)).reshape([-1 if axis == dim else 1 for axis in range(array.ndim)]) for dim in (source, target)]
    chosen = jax.random.permutation(key, parts)[partner]
    strong = (owner == chosen) | (owner == (partner + parts // 2) % parts)
    return jnp.where(strong, factor * array, array)


def steps_of(own_key, shape, pieces, least, largest):
    def one(position, blocks):
        heights = jax.random.uniform(jax.random.fold_in(jax.random.fold_in(own_key, 6), position), (blocks,), jnp.float32, least / len(pieces), largest / len(pieces))
        return jnp.repeat(jnp.exp(heights), shape[position] // blocks).reshape((-1,) + (1,) * (len(shape) - position - 1))

    factor_of = one(*pieces[0])
    for cut in pieces[1:]:
        factor_of = factor_of * one(*cut)
    return factor_of


def centred(own_key, extent, width, most, shards=(), held_as=jnp.bfloat16):
    entries = jax.random.normal(own_key, extent, jnp.float32) * width
    if len(shards) > 0:
        entries = steps_of(own_key, extent, shards, -0.22, 0.18) * entries
    return jnp.clip(entries, min=-most, max=most).astype(held_as)


def bell_draw_with(rng, extent, deviation, bound, shards, heavy, kind=jnp.bfloat16):
    result = deviation * jax.random.normal(rng, extent, jnp.float32)
    if shards:
        result = result * steps_of(rng, extent, shards, -0.22, 0.18)
    return jnp.clip(spiked(result, jax.random.fold_in(rng, 3), *heavy), -bound, bound).astype(kind)


def setup_inputs(seed: int = 0, part: int = 0) -> dict:
    keys = jax.random.split(jax.random.key(seed), 11)
    part_splits = jax.random.split(jax.random.fold_in(keys[10], part), 11)
    mixer_input = centred(part_splits[0], (SEQUENCE_LENGTH, INNER), 1.0, 6.0, ((0, 4), (1, 4)))
    state_maps = centred(part_splits[1], (SEQUENCE_LENGTH, 2 * STATE), 1.0, 6.0, ((0, 4),))
    gate_input = centred(part_splits[2], (SEQUENCE_LENGTH, INNER), 1.0, 6.0, ((0, 4), (1, 4)))
    step_raw = draw_step_raw(jax.random.fold_in(jax.random.fold_in(keys[10], part), 71), part)
    decay_log = jnp.clip(-4.0 + 2.0 * jax.random.uniform(keys[4], (HEAD_TOTAL,), jnp.float32) ** steps_of(keys[4], (HEAD_TOTAL,), ((0, 4),), -0.2, 0.2), -4.0, -2.0)
    skip_gain = jnp.clip(0.5 + 1.0 * jax.random.uniform(keys[5], (HEAD_TOTAL,), jnp.float32) ** steps_of(keys[5], (HEAD_TOTAL,), ((0, 4),), -0.2, 0.2), 0.5, 1.5)
    conv_input = centred(keys[6], (CONV, INNER), CONV ** -0.5, 3.0, ((1, 4),))
    conv_maps = centred(keys[7], (CONV, 2 * STATE), CONV ** -0.5, 3.0)
    norm_gain = jnp.clip(1.0 + 0.18 * jax.random.normal(keys[8], (INNER,), jnp.float32), 0.1, 1.9)
    out_weight = bell_draw_with(keys[9], (INNER, D), INNER ** -0.5, 0.09375, ((0, 4),), (0, 1, 4, 2.0))
    return dict(mixer_input=mixer_input, state_maps=state_maps, gate_input=gate_input, step_raw=step_raw, decay_log=decay_log, skip_gain=skip_gain, conv_input=conv_input, conv_maps=conv_maps, norm_gain=norm_gain, out_weight=out_weight)


PRECISE = lax.Precision.HIGHEST

def causal_conv(values, kernel):
    widened = values.astype(jnp.float32)
    padded = jnp.concatenate([jnp.zeros((CONV - 1, widened.shape[1]), jnp.float32), widened], axis=0)
    summed = jnp.zeros(widened.shape, jnp.float32)
    for offset in range(CONV):
        summed = summed + kernel[offset].astype(jnp.float32) * padded[offset:offset + widened.shape[0]]
    return jax.nn.silu(summed).astype(jnp.bfloat16)

def reference(mixer_input, state_maps, gate_input, step_raw, decay_log, skip_gain, conv_input, conv_maps, norm_gain, out_weight):
    conv_out = causal_conv(mixer_input, conv_input)
    maps_out = causal_conv(state_maps, conv_maps)
    blocks = SEQUENCE_LENGTH // SPAN
    b_blocks = maps_out[:, :STATE].astype(jnp.float32).reshape(blocks, SPAN, STATE)
    c_blocks = maps_out[:, STATE:].astype(jnp.float32).reshape(blocks, SPAN, STATE)
    scores = jnp.einsum('ktn,ksn->kts', c_blocks, b_blocks, precision=PRECISE)
    step_size = jax.nn.softplus(step_raw)
    rates = jnp.exp(decay_log)
    causal = jnp.arange(SPAN)[:, None] >= jnp.arange(SPAN)[None, :]
    heads_first = conv_out.reshape(SEQUENCE_LENGTH, HEAD_TOTAL, HEAD_DIM).transpose(1, 0, 2)

    def one_head(operands):
        values, step_sizes, decay_rate, skip_scale = operands
        log_decay = -decay_rate * step_sizes
        cumulative = jnp.cumsum(log_decay.reshape(blocks, SPAN), axis=1)
        step_blocks = step_sizes.reshape(blocks, SPAN)
        value_blocks = values.astype(jnp.float32).reshape(blocks, SPAN, HEAD_DIM)
        logarithm_spacing = jnp.where(causal, cumulative[:, :, None] - cumulative[:, None, :], 0.0)
        weights = jnp.where(causal, scores * jnp.exp(logarithm_spacing) * step_blocks[:, None, :], 0.0).astype(jnp.bfloat16)
        inside = jnp.einsum('kts,ksp->ktp', weights.astype(jnp.float32), value_blocks, precision=PRECISE)
        tail_weight = jnp.exp(cumulative[:, -1:] - cumulative) * step_blocks
        block_states = jnp.einsum('ksp,ksn->kpn', value_blocks * tail_weight[:, :, None], b_blocks, precision=PRECISE)

        def advance(state_now, element):
            decay_now, block_add = element
            return (decay_now * state_now + block_add, state_now)
        _, carried = lax.scan(advance, jnp.zeros((HEAD_DIM, STATE), jnp.float32), (jnp.exp(cumulative[:, -1]), block_states))
        carried_part = jnp.einsum('ktn,kpn->ktp', c_blocks, carried, precision=PRECISE) * jnp.exp(cumulative)[:, :, None]
        return (inside + carried_part + skip_scale * value_blocks).reshape(SEQUENCE_LENGTH, HEAD_DIM)
    scanned = lax.map(one_head, (heads_first, step_size, rates, skip_gain))
    scanned = scanned.transpose(1, 0, 2).reshape(SEQUENCE_LENGTH, INNER)
    gated_values = scanned * jax.nn.silu(gate_input.astype(jnp.float32))
    grouped = gated_values.reshape(SEQUENCE_LENGTH, HEAD_TOTAL, HEAD_DIM)
    inverse_root_mean = lax.rsqrt(lax.optimization_barrier(jnp.mean(grouped * grouped, axis=2, keepdims=True)) + 1e-05)
    normed = ((grouped * inverse_root_mean).reshape(SEQUENCE_LENGTH, INNER) * norm_gain).astype(jnp.bfloat16)
    return jnp.dot(normed, out_weight, preferred_element_type=jnp.float32).astype(jnp.bfloat16)
```

```python
import functools

import jax
import jax.numpy as jnp
from jax import lax
from jax.experimental import pallas as pl
from jax.experimental.pallas import tpu as pltpu
from jax.sharding import PartitionSpec as P

MESH = pl.DeviceIdType.MESH
LOG2E = 1.4426950408889634
NEG = -1e30
LANES = 128
F32 = jnp.float32
BF16 = jnp.bfloat16


def silu(v):
    return 0.5 * v * (1.0 + jnp.tanh(0.5 * v))


def iota(shape, dim):
    return lax.broadcasted_iota(jnp.int32, shape, dim)


def dot(a, b, **kw):
    return jnp.dot(a, b, preferred_element_type=F32, **kw)


def kernel(
    sizes,
    x,
    maps,
    gate,
    step,
    decay,
    skip,
    taps,
    map_taps,
    gain,
    w_hbm,
    out,
    halo_x,
    halo_m,
    wide,
    conv,
    rows,
    decay_row,
    state,
    state_in,
    state_out,
    local_part,
    growth,
    normed,
    partial,
    from_left,
    from_right,
    wbuf,
    halo_sem,
    state_sem,
    w_sem,
    send_right,
    recv_right,
    send_left,
    recv_left,
):
    T, S, hd, np_, pw, nbuf = sizes
    tokens, C = x.shape
    half = tokens // 2
    Hp = step.shape[0]
    N = maps.shape[1] // 2
    lead = taps.shape[0] - 1
    tail = halo_x.shape[0]
    cols = np_ * pw
    total = T * np_
    m = lax.axis_index("tensor")
    me = lax.axis_index("seq")

    def piece_of(i):
        k, q = lax.div(i, np_), lax.rem(i, np_)
        return jnp.where(2 * m < T, T - 1 - k, k), q

    def w_copy(i, slot):
        c, q = piece_of(i)
        start = pl.multiple_of((c * np_ + q) * pw, pw)
        return pltpu.make_async_copy(w_hbm.at[:, pl.ds(start, pw)], wbuf.at[slot], w_sem.at[slot])

    for i in range(nbuf):
        w_copy(jnp.int32(i), i).start()

    barrier = pltpu.get_barrier_semaphore()
    for axis, mine, count in (("seq", me, S), ("tensor", m, T)):
        for other in (lax.rem(mine + 1, count), lax.rem(mine + count - 1, count)):
            pl.semaphore_signal(barrier, inc=1, device_id={axis: other}, device_id_type=MESH)
    pl.semaphore_wait(barrier, 4)

    after = lax.rem(me + 1, S)

    def halo_copies():
        return [
            pltpu.make_async_remote_copy(
                src_ref=src.at[pl.ds(tokens - tail, tail), :],
                dst_ref=dst,
                send_sem=halo_sem.at[0, k],
                recv_sem=halo_sem.at[1, k],
                device_id={"seq": after},
                device_id_type=MESH,
            )
            for k, (src, dst) in enumerate(((x, halo_x), (maps, halo_m)))
        ]

    @pl.when(me < S - 1)
    def _():
        for copy in halo_copies():
            copy.start()

    raw = step[...]
    size = jnp.maximum(raw, 0.0) + jnp.log1p(jnp.exp(-jnp.abs(raw)))
    log_decay = (-LOG2E * jnp.exp(decay[...])) * size
    upto = (iota((tokens, tokens), 0) <= iota((tokens, tokens), 1)).astype(F32)
    cum = dot(log_decay, upto, precision=lax.Precision.HIGHEST)
    shifted = cum - jnp.log(size) * LOG2E
    rows[...] = shifted
    last = cum[:, tokens - 1 : tokens]
    tail_weight = jnp.exp2(last - shifted)
    head_decay = jnp.exp2(last)
    hi = cum.astype(BF16).astype(F32)
    mid = (cum - hi).astype(BF16).astype(F32)
    low = cum - hi - mid
    spread = jnp.transpose(jnp.concatenate([hi, mid, low, tail_weight], axis=0)).astype(BF16)

    def in_head(count, width, start, group):
        offset = iota((count, width), 1) + start - (iota((count, width), 0) - group * Hp) * hd
        return (offset >= 0) & (offset < hd)

    def convolve(values, halo, kernel_taps, width):
        wide[0:8, :width] = halo
        wide[8:, :width] = values.astype(F32)
        k = kernel_taps.astype(F32)
        summed = k[0:1] * wide[8 - lead : 8 - lead + tokens, :width]
        for o in range(1, lead + 1):
            summed = summed + k[o : o + 1] * wide[8 - lead + o : 8 - lead + o + tokens, :width]
        return silu(summed)

    @pl.when(me > 0)
    def _():
        for copy in halo_copies():
            copy.wait_recv()

    @pl.when(me == 0)
    def _():
        halo_x[...] = jnp.zeros_like(halo_x)
        halo_m[...] = jnp.zeros_like(halo_m)
        state_in[...] = jnp.zeros_like(state_in)

    maps_out = convolve(maps[...], halo_m[...].astype(F32)[tail - 8 :], map_taps[...], 2 * N)
    b_t = jnp.transpose(maps_out[:, :N]).astype(BF16)
    c_mat = maps_out[:, N:].astype(BF16)
    scores = dot(c_mat, b_t)

    cw = min(C, 256)

    def states(i, carry):
        start = pl.multiple_of(i * cw, cw)
        ds = pl.ds(start, cw)
        value = convolve(x[:, ds], halo_x[:, ds].astype(F32)[tail - 8 :], taps[:, ds], cw).astype(
            BF16
        )
        conv[:, ds] = value
        spread_tail = dot(spread, in_head(4 * Hp, cw, start, 3).astype(BF16))
        weighted = (value.astype(F32) * spread_tail).astype(BF16)
        own = dot(b_t, weighted)
        state[:, ds] = own
        decay_row[:, ds] = jnp.sum(
            jnp.where(in_head(Hp, cw, start, 0), head_decay, 0.0), axis=0, keepdims=True
        )
        state_out[:, ds] = own.astype(BF16)
        return carry

    lax.fori_loop(0, C // cw, states, 0)

    def state_copy():
        return pltpu.make_async_remote_copy(
            src_ref=state_out,
            dst_ref=state_in,
            send_sem=state_sem.at[0],
            recv_sem=state_sem.at[1],
            device_id={"seq": after},
            device_id_type=MESH,
        )

    def relay():
        state_copy().wait_recv()

        @pl.when(me < S - 1)
        def _():
            state_out[...] = (decay_row[...] * state_in[...].astype(F32) + state[...]).astype(BF16)
            state_copy().start()

    @pl.when((me == 0) & (me < S - 1))
    def _():
        state_copy().start()

    @pl.when(me == 1)
    def _():
        relay()

    triangle = iota((half, half), 0) >= iota((half, half), 1)
    per = LANES // hd

    def inside(p, carry):
        start = pl.multiple_of(p * LANES, LANES)
        ds = pl.ds(start, LANES)
        member = (
            in_head(4 * Hp, LANES, start, 0)
            | in_head(4 * Hp, LANES, start, 1)
            | in_head(4 * Hp, LANES, start, 2)
        )
        column = dot(spread, member.astype(BF16))
        value = conv[:, ds].astype(F32)
        lane = iota((tokens, LANES), 1)
        top = jnp.zeros((half, LANES), F32)
        bottom = jnp.zeros((half, LANES), F32)
        for j in range(per):
            row = rows[pl.ds(p * per + j, 1), :]
            mine = column[:, j * hd : j * hd + 1]
            own = jnp.where((lane >= j * hd) & (lane < (j + 1) * hd), value, 0.0).astype(BF16)
            first = jnp.where(triangle, mine[:half] - row[:, :half], NEG)
            w_first = (scores[:half, :half] * jnp.exp2(first)).astype(BF16)
            top = top + dot(w_first, own[:half])
            w_left = (scores[half:, :half] * jnp.exp2(mine[half:] - row[:, :half])).astype(BF16)
            second = jnp.where(triangle, mine[half:] - row[:, half:], NEG)
            w_right = (scores[half:, half:] * jnp.exp2(second)).astype(BF16)
            bottom = bottom + dot(w_left, own[:half]) + dot(w_right, own[half:])
        skip_row = jnp.sum(
            jnp.where(in_head(Hp, LANES, start, 0), skip[...], 0.0), axis=0, keepdims=True
        )
        gated = silu(gate[:, ds].astype(F32))
        joined = jnp.concatenate([top, bottom], axis=0)
        local_part[:, ds] = (joined + skip_row * value) * gated
        growth[:, ds] = jnp.exp2(column) * gated
        return carry

    lax.fori_loop(0, C // LANES, inside, 0)

    @pl.when(me > 1)
    def _():
        relay()

    same_head = None
    for j in range(per):
        block = lambda d: (iota((LANES, LANES), d) >= j * hd) & (
            iota((LANES, LANES), d) < (j + 1) * hd
        )
        both = block(0) & block(1)
        same_head = both if same_head is None else same_head | both
    same_head = same_head.astype(BF16)

    def finish(p, carry):
        ds = pl.ds(pl.multiple_of(p * LANES, LANES), LANES)
        y = local_part[:, ds] + dot(c_mat, state_in[:, ds]) * growth[:, ds]
        mean = dot((y * y).astype(BF16), same_head) * (1.0 / hd)
        normed[:, ds] = (y * lax.rsqrt(mean + 1e-05) * gain[:, ds]).astype(BF16)
        return carry

    lax.fori_loop(0, C // LANES, finish, 0)

    right, left = lax.rem(m + 1, T), lax.rem(m + T - 1, T)

    def send(rightward, slot, index):
        buffer, ssem, rsem, to = (
            (from_left, send_right, recv_right, right)
            if rightward
            else (from_right, send_left, recv_left, left)
        )
        return pltpu.make_async_remote_copy(
            src_ref=partial.at[index],
            dst_ref=buffer.at[slot],
            send_sem=ssem.at[slot],
            recv_sem=rsem.at[slot],
            device_id={"tensor": to},
            device_id_type=MESH,
        )

    def project(i, carry):
        slot = lax.rem(i, nbuf)
        c, q = piece_of(i)
        index = c * np_ + q
        w_copy(i, slot).wait()
        result = dot(normed[...], wbuf[slot]).astype(BF16)

        @pl.when(c == m)
        def _():
            out[:, pl.ds(pl.multiple_of(q * pw, pw), pw)] = result

        @pl.when(c != m)
        def _():
            partial[index] = result

        @pl.when((m == 0) & (c != m))
        def _():
            send(True, i, index).start()

        @pl.when((m == T - 1) & (c != m))
        def _():
            send(False, i, index).start()

        @pl.when(i + nbuf < total)
        def _():
            w_copy(i + nbuf, slot).start()

        return carry

    lax.fori_loop(0, total, project, 0)

    def arrive(rightward, slot, buffer):
        k, q = lax.div(slot, np_), lax.rem(slot, np_)
        c = T - 1 - k if rightward else k
        index = c * np_ + q
        send(rightward, slot, index).wait_recv()

        @pl.when(c == m)
        def _():
            ds = pl.ds(pl.multiple_of(q * pw, pw), pw)
            out[:, ds] = (out[:, ds].astype(F32) + buffer[slot].astype(F32)).astype(BF16)

        @pl.when(c != m)
        def _():
            partial[index] = (partial[index].astype(F32) + buffer[slot].astype(F32)).astype(BF16)
            send(rightward, slot, index).start()

    def exchange(t, carry):
        to_right = t - m
        to_left = t - (T - 1 - m)

        @pl.when((m > 0) & (to_right >= 0) & (to_right < (T - m) * np_))
        def _():
            arrive(True, to_right, from_left)

        @pl.when((m < T - 1) & (to_left >= 0) & (to_left < (m + 1) * np_))
        def _():
            arrive(False, to_left, from_right)

        return carry

    lax.fori_loop(1, total + 1, exchange, 0)

    def drain(slot, carry):
        @pl.when(slot < (T - 1 - m) * np_)
        def _():
            send(True, slot, 0).wait_send()

        @pl.when(slot < m * np_)
        def _():
            send(False, slot, 0).wait_send()

        return carry

    lax.fori_loop(0, total, drain, 0)

    @pl.when(me < S - 1)
    def _():
        for copy in halo_copies():
            copy.wait_send()
        state_copy().wait_send()


def local(
    sizes,
    mixer_input,
    state_maps,
    gate_input,
    step_raw,
    decay_log,
    skip_gain,
    conv_input,
    conv_maps,
    norm_gain,
    out_weight,
):
    T, S = sizes
    tokens, C = mixer_input.shape
    H = decay_log.shape[0]
    hd = C // H
    two_n = state_maps.shape[1]
    n = two_n // 2
    cols = out_weight.shape[1] // T
    pw = min(cols, 512)
    np_ = cols // pw
    total = T * np_
    nbuf = min(4, total)
    pad = -H % 8
    column = lambda a: jnp.pad(a, (0, pad)).reshape(H + pad, 1)
    Hp = H + pad
    vmem = pl.BlockSpec(memory_space=pltpu.VMEM)
    dma = pltpu.SemaphoreType.DMA
    return pl.pallas_call(
        functools.partial(kernel, (T, S, hd, np_, pw, nbuf)),
        out_shape=jax.ShapeDtypeStruct((tokens, cols), BF16),
        in_specs=[vmem] * 9 + [pl.BlockSpec(memory_space=pl.ANY)],
        out_specs=vmem,
        scratch_shapes=[
            pltpu.VMEM((16, C), BF16),
            pltpu.VMEM((16, two_n), BF16),
            pltpu.VMEM((tokens + 8, max(two_n, min(C, 256))), F32),
            pltpu.VMEM((tokens, C), BF16),
            pltpu.VMEM((Hp, tokens), F32),
            pltpu.VMEM((1, C), F32),
            pltpu.VMEM((n, C), F32),
            pltpu.VMEM((n, C), BF16),
            pltpu.VMEM((n, C), BF16),
            pltpu.VMEM((tokens, C), F32),
            pltpu.VMEM((tokens, C), F32),
            pltpu.VMEM((tokens, C), BF16),
            pltpu.VMEM((total, tokens, pw), BF16),
            pltpu.VMEM((total, tokens, pw), BF16),
            pltpu.VMEM((total, tokens, pw), BF16),
            pltpu.VMEM((nbuf, C, pw), BF16),
            dma((2, 2)),
            dma((2,)),
            dma((nbuf,)),
            dma((total,)),
            dma((total,)),
            dma((total,)),
            dma((total,)),
        ],
        compiler_params=pltpu.CompilerParams(
            collective_id=0, has_side_effects=True, vmem_limit_bytes=60 * 1024 * 1024
        ),
    )(
        mixer_input,
        state_maps,
        gate_input,
        jnp.pad(step_raw, ((0, pad), (0, 0))),
        column(decay_log),
        column(skip_gain),
        conv_input,
        conv_maps,
        norm_gain.reshape(1, C),
        out_weight,
    )


def solution(mesh):
    placed = (
        P(("group", "seq"), "tensor"),
        P(("group", "seq"), None),
        P(("group", "seq"), "tensor"),
        P("tensor", ("group", "seq")),
        P("tensor"),
        P("tensor"),
        P(None, "tensor"),
        P(),
        P("tensor"),
        P("tensor", None),
    )
    return jax.shard_map(
        functools.partial(local, (mesh.shape["tensor"], mesh.shape["seq"])),
        mesh=mesh,
        in_specs=placed,
        out_specs=P(("group", "seq"), "tensor"),
        check_vma=False,
    )
```

```python
import functools

import jax
import jax.numpy as jnp
from jax import lax
from jax.experimental import pallas as pl
from jax.experimental.pallas import tpu as pltpu
from jax.sharding import PartitionSpec as P

MESH = pl.DeviceIdType.MESH
LOG2E = 1.4426950408889634
NEG = -1e30
LANES = 128
F32 = jnp.float32
BF16 = jnp.bfloat16


def silu(v):
    return 0.5 * v * (1.0 + jnp.tanh(0.5 * v))


def iota(shape, dim):
    return lax.broadcasted_iota(jnp.int32, shape, dim)


def dot(a, b, **kw):
    return jnp.dot(a, b, preferred_element_type=F32, **kw)


def kernel(
    sizes,
    *refs,
):
    sources, w_hbm, out, held = refs[:9], refs[9], refs[10], refs[11:20]
    x, maps, gate, step, decay, skip, taps, map_taps, gain = held
    (
        halo_x,
        halo_m,
        wide,
        conv,
        rows,
        decay_row,
        state,
        state_in,
        state_out,
        local_part,
        growth,
        normed,
        partial,
        from_left,
        from_right,
        wbuf,
        halo_sem,
        state_sem,
        w_sem,
        send_right,
        recv_right,
        send_left,
        recv_left,
        in_sem,
    ) = refs[20:]
    T, S, hd, np_, pw, nbuf = sizes
    tokens, C = x.shape
    half = tokens // 2
    Hp = step.shape[0]
    N = maps.shape[1] // 2
    lead = taps.shape[0] - 1
    tail = halo_x.shape[0]
    cols = np_ * pw
    total = T * np_
    m = lax.axis_index("tensor")
    me = lax.axis_index("seq")

    def piece_of(i):
        k, q = lax.div(i, np_), lax.rem(i, np_)
        return jnp.where(2 * m < T, T - 1 - k, k), q

    def w_copy(i, slot):
        c, q = piece_of(i)
        start = pl.multiple_of((c * np_ + q) * pw, pw)
        return pltpu.make_async_copy(w_hbm.at[:, pl.ds(start, pw)], wbuf.at[slot], w_sem.at[slot])

    loads = [
        pltpu.make_async_copy(src, dst, in_sem.at[k]) for k, (src, dst) in enumerate(zip(sources, held))
    ]
    for load in loads:
        load.start()
    for i in range(nbuf):
        w_copy(jnp.int32(i), i).start()

    barrier = pltpu.get_barrier_semaphore()
    for axis, mine, count in (("seq", me, S), ("tensor", m, T)):
        for other in (lax.rem(mine + 1, count), lax.rem(mine + count - 1, count)):
            pl.semaphore_signal(barrier, inc=1, device_id={axis: other}, device_id_type=MESH)
    pl.semaphore_wait(barrier, 4)

    after = lax.rem(me + 1, S)
    for load in loads:
        load.wait()

    def halo_copies():
        return [
            pltpu.make_async_remote_copy(
                src_ref=src.at[pl.ds(tokens - tail, tail), :],
                dst_ref=dst,
                send_sem=halo_sem.at[0, k],
                recv_sem=halo_sem.at[1, k],
                device_id={"seq": after},
                device_id_type=MESH,
            )
            for k, (src, dst) in enumerate(((x, halo_x), (maps, halo_m)))
        ]

    @pl.when(me < S - 1)
    def _():
        for copy in halo_copies():
            copy.start()

    def upright(row):
        heads = row.shape[1]
        return jnp.sum(
            jnp.where(iota((Hp, heads), 0) == iota((Hp, heads), 1), row[...], 0.0),
            axis=1,
            keepdims=True,
        )

    raw = step[...]
    size = jnp.maximum(raw, 0.0) + jnp.log1p(jnp.exp(-jnp.abs(raw)))
    log_decay = (-LOG2E * jnp.exp(upright(decay))) * size
    upto = (iota((tokens, tokens), 0) <= iota((tokens, tokens), 1)).astype(F32)
    cum = dot(log_decay, upto, precision=lax.Precision.HIGHEST)
    shifted = cum - jnp.log(size) * LOG2E
    rows[...] = shifted
    skips = upright(skip)
    last = cum[:, tokens - 1 : tokens]
    tail_weight = jnp.exp2(last - shifted)
    head_decay = jnp.exp2(last)
    hi = cum.astype(BF16).astype(F32)
    mid = (cum - hi).astype(BF16).astype(F32)
    low = cum - hi - mid
    spread = jnp.transpose(jnp.concatenate([hi, mid, low, tail_weight], axis=0)).astype(BF16)

    def in_head(count, width, start, group):
        offset = iota((count, width), 1) + start - (iota((count, width), 0) - group * Hp) * hd
        return (offset >= 0) & (offset < hd)

    def convolve(values, halo, kernel_taps, width):
        wide[0:8, :width] = halo
        wide[8:, :width] = values.astype(F32)
        k = kernel_taps.astype(F32)
        summed = k[0:1] * wide[8 - lead : 8 - lead + tokens, :width]
        for o in range(1, lead + 1):
            summed = summed + k[o : o + 1] * wide[8 - lead + o : 8 - lead + o + tokens, :width]
        return silu(summed)

    @pl.when(me > 0)
    def _():
        for copy in halo_copies():
            copy.wait_recv()

    @pl.when(me == 0)
    def _():
        halo_x[...] = jnp.zeros_like(halo_x)
        halo_m[...] = jnp.zeros_like(halo_m)
        state_in[...] = jnp.zeros_like(state_in)

    maps_out = convolve(maps[...], halo_m[...].astype(F32)[tail - 8 :], map_taps[...], 2 * N)
    b_t = jnp.transpose(maps_out[:, :N]).astype(BF16)
    c_mat = maps_out[:, N:].astype(BF16)
    scores = dot(c_mat, b_t)

    cw = state.shape[2]
    chunks = C // cw

    def state_copy(i):
        return pltpu.make_async_remote_copy(
            src_ref=state_out.at[i],
            dst_ref=state_in.at[i],
            send_sem=state_sem.at[0, i],
            recv_sem=state_sem.at[1, i],
            device_id={"seq": after},
            device_id_type=MESH,
        )

    def relay(i):
        state_copy(i).wait_recv()

        @pl.when(me < S - 1)
        def _():
            decayed = decay_row[:, pl.ds(pl.multiple_of(i * cw, cw), cw)]
            state_out[i] = (decayed * state_in[i].astype(F32) + state[i]).astype(BF16)
            state_copy(i).start()

    def states(i, carry):
        start = pl.multiple_of(i * cw, cw)
        ds = pl.ds(start, cw)
        value = convolve(x[:, ds], halo_x[:, ds].astype(F32)[tail - 8 :], taps[:, ds], cw).astype(
            BF16
        )
        conv[:, ds] = value
        spread_tail = dot(spread, in_head(4 * Hp, cw, start, 3).astype(BF16))
        weighted = (value.astype(F32) * spread_tail).astype(BF16)
        own = dot(b_t, weighted)
        decay_row[:, ds] = jnp.sum(
            jnp.where(in_head(Hp, cw, start, 0), head_decay, 0.0), axis=0, keepdims=True
        )

        @pl.when(me > 0)
        def _():
            state[i] = own

        @pl.when((me == 0) & (me < S - 1))
        def _():
            state_out[i] = own.astype(BF16)
            state_copy(i).start()

        @pl.when((me == 1) & (i > 0))
        def _():
            relay(jnp.maximum(i - 1, 0))

        return carry

    lax.fori_loop(0, chunks, states, 0)

    @pl.when(me == 1)
    def _():
        relay(chunks - 1)

    triangle = iota((half, half), 0) >= iota((half, half), 1)
    per = LANES // hd

    def inside(p, carry):
        start = pl.multiple_of(p * LANES, LANES)
        ds = pl.ds(start, LANES)
        member = (
            in_head(4 * Hp, LANES, start, 0)
            | in_head(4 * Hp, LANES, start, 1)
            | in_head(4 * Hp, LANES, start, 2)
        )
        column = dot(spread, member.astype(BF16))
        value = conv[:, ds].astype(F32)
        lane = iota((tokens, LANES), 1)
        top = jnp.zeros((half, LANES), F32)
        bottom = jnp.zeros((half, LANES), F32)
        for j in range(per):
            row = rows[pl.ds(p * per + j, 1), :]
            mine = column[:, j * hd : j * hd + 1]
            own = jnp.where((lane >= j * hd) & (lane < (j + 1) * hd), value, 0.0).astype(BF16)
            first = jnp.where(triangle, mine[:half] - row[:, :half], NEG)
            w_first = (scores[:half, :half] * jnp.exp2(first)).astype(BF16)
            top = top + dot(w_first, own[:half])
            w_left = (scores[half:, :half] * jnp.exp2(mine[half:] - row[:, :half])).astype(BF16)
            second = jnp.where(triangle, mine[half:] - row[:, half:], NEG)
            w_right = (scores[half:, half:] * jnp.exp2(second)).astype(BF16)
            bottom = bottom + dot(w_left, own[:half]) + dot(w_right, own[half:])
        skip_row = jnp.sum(
            jnp.where(in_head(Hp, LANES, start, 0), skips, 0.0), axis=0, keepdims=True
        )
        gated = silu(gate[:, ds].astype(F32))
        joined = jnp.concatenate([top, bottom], axis=0)
        local_part[:, ds] = (joined + skip_row * value) * gated
        growth[:, ds] = jnp.exp2(column) * gated
        return carry

    lax.fori_loop(0, C // LANES, inside, 0)

    same_head = None
    for j in range(per):
        block = lambda d: (iota((LANES, LANES), d) >= j * hd) & (
            iota((LANES, LANES), d) < (j + 1) * hd
        )
        both = block(0) & block(1)
        same_head = both if same_head is None else same_head | both
    same_head = same_head.astype(BF16)

    def finish(i, carry):
        @pl.when(me > 1)
        def _():
            relay(i)

        for k in range(0, cw, LANES):
            ds = pl.ds(pl.multiple_of(i * cw + k, LANES), LANES)
            incoming = dot(c_mat, state_in[i, :, k : k + LANES])
            y = local_part[:, ds] + incoming * growth[:, ds]
            mean = dot((y * y).astype(BF16), same_head) * (1.0 / hd)
            normed[:, ds] = (y * lax.rsqrt(mean + 1e-05) * gain[:, ds]).astype(BF16)
        return carry

    lax.fori_loop(0, chunks, finish, 0)

    right, left = lax.rem(m + 1, T), lax.rem(m + T - 1, T)

    def send(rightward, slot, index):
        buffer, ssem, rsem, to = (
            (from_left, send_right, recv_right, right)
            if rightward
            else (from_right, send_left, recv_left, left)
        )
        return pltpu.make_async_remote_copy(
            src_ref=partial.at[index],
            dst_ref=buffer.at[slot],
            send_sem=ssem.at[slot],
            recv_sem=rsem.at[slot],
            device_id={"tensor": to},
            device_id_type=MESH,
        )

    def project(i, carry):
        slot = lax.rem(i, nbuf)
        c, q = piece_of(i)
        index = c * np_ + q
        w_copy(i, slot).wait()
        result = dot(normed[...], wbuf[slot]).astype(BF16)

        @pl.when(c == m)
        def _():
            out[:, pl.ds(pl.multiple_of(q * pw, pw), pw)] = result

        @pl.when(c != m)
        def _():
            partial[index] = result

        @pl.when((m == 0) & (c != m))
        def _():
            send(True, i, index).start()

        @pl.when((m == T - 1) & (c != m))
        def _():
            send(False, i, index).start()

        @pl.when(i + nbuf < total)
        def _():
            w_copy(i + nbuf, slot).start()

        return carry

    lax.fori_loop(0, total, project, 0)

    def arrive(rightward, slot, buffer):
        k, q = lax.div(slot, np_), lax.rem(slot, np_)
        c = T - 1 - k if rightward else k
        index = c * np_ + q
        send(rightward, slot, index).wait_recv()

        @pl.when(c == m)
        def _():
            ds = pl.ds(pl.multiple_of(q * pw, pw), pw)
            out[:, ds] = (out[:, ds].astype(F32) + buffer[slot].astype(F32)).astype(BF16)

        @pl.when(c != m)
        def _():
            partial[index] = (partial[index].astype(F32) + buffer[slot].astype(F32)).astype(BF16)
            send(rightward, slot, index).start()

    def exchange(t, carry):
        to_right = t - m
        to_left = t - (T - 1 - m)

        @pl.when((m > 0) & (to_right >= 0) & (to_right < (T - m) * np_))
        def _():
            arrive(True, to_right, from_left)

        @pl.when((m < T - 1) & (to_left >= 0) & (to_left < (m + 1) * np_))
        def _():
            arrive(False, to_left, from_right)

        return carry

    lax.fori_loop(1, total + 1, exchange, 0)

    def drain(slot, carry):
        @pl.when(slot < (T - 1 - m) * np_)
        def _():
            send(True, slot, 0).wait_send()

        @pl.when(slot < m * np_)
        def _():
            send(False, slot, 0).wait_send()

        return carry

    lax.fori_loop(0, total, drain, 0)

    @pl.when(me < S - 1)
    def _():
        for copy in halo_copies():
            copy.wait_send()
        for i in range(chunks):
            state_copy(i).wait_send()


def local(
    sizes,
    mixer_input,
    state_maps,
    gate_input,
    step_raw,
    decay_log,
    skip_gain,
    conv_input,
    conv_maps,
    norm_gain,
    out_weight,
):
    T, S = sizes
    tokens, C = mixer_input.shape
    H = decay_log.shape[0]
    hd = C // H
    two_n = state_maps.shape[1]
    n = two_n // 2
    cols = out_weight.shape[1] // T
    pw = min(cols, 512)
    np_ = cols // pw
    total = T * np_
    nbuf = min(4, total)
    pad = -H % 8
    cw = min(C, 256)
    Hp = H + pad
    operands = (
        mixer_input,
        state_maps,
        gate_input,
        jnp.pad(step_raw, ((0, pad), (0, 0))),
        decay_log.reshape(1, H),
        skip_gain.reshape(1, H),
        conv_input,
        conv_maps,
        norm_gain.reshape(1, C),
        out_weight,
    )
    vmem = pl.BlockSpec(memory_space=pltpu.VMEM)
    dma = pltpu.SemaphoreType.DMA
    return pl.pallas_call(
        functools.partial(kernel, (T, S, hd, np_, pw, nbuf)),
        out_shape=pltpu.VMEM((tokens, cols), BF16),
        in_specs=[pl.BlockSpec(memory_space=pltpu.HBM)] * 10,
        out_specs=vmem,
        scratch_shapes=[pltpu.VMEM(a.shape, a.dtype) for a in operands[:9]]
        + [
            pltpu.VMEM((16, C), BF16),
            pltpu.VMEM((16, two_n), BF16),
            pltpu.VMEM((tokens + 8, max(two_n, cw)), F32),
            pltpu.VMEM((tokens, C), BF16),
            pltpu.VMEM((Hp, tokens), F32),
            pltpu.VMEM((1, C), F32),
            pltpu.VMEM((C // cw, n, cw), F32),
            pltpu.VMEM((C // cw, n, cw), BF16),
            pltpu.VMEM((C // cw, n, cw), BF16),
            pltpu.VMEM((tokens, C), F32),
            pltpu.VMEM((tokens, C), F32),
            pltpu.VMEM((tokens, C), BF16),
            pltpu.VMEM((total, tokens, pw), BF16),
            pltpu.VMEM((total, tokens, pw), BF16),
            pltpu.VMEM((total, tokens, pw), BF16),
            pltpu.VMEM((nbuf, C, pw), BF16),
            dma((2, 2)),
            dma((2, C // cw)),
            dma((nbuf,)),
            dma((total,)),
            dma((total,)),
            dma((total,)),
            dma((total,)),
            dma((9,)),
        ],
        compiler_params=pltpu.CompilerParams(
            collective_id=0, has_side_effects=True, vmem_limit_bytes=65900000
        ),
    )(*operands)


def solution(mesh):
    placed = (
        P(("group", "seq"), "tensor"),
        P(("group", "seq"), None),
        P(("group", "seq"), "tensor"),
        P("tensor", ("group", "seq")),
        P("tensor"),
        P("tensor"),
        P(None, "tensor"),
        P(),
        P("tensor"),
        P("tensor", None),
    )
    return jax.shard_map(
        functools.partial(local, (mesh.shape["tensor"], mesh.shape["seq"])),
        mesh=mesh,
        in_specs=placed,
        out_specs=P(("group", "seq"), "tensor"),
        check_vma=False,
    )
```
